8 devices in a mesh: rep: 1 (over z), dp: 8 (over x, y, core).
Axes of the slice: x: 2, y: 2, z: 1, core: 2. Of those that a mesh axis runs over, the one named last changes fastest.
Arguments:
- x: bfloat16 [8, 2048, 1280], P(('rep', 'dp'))
- dy: bfloat16 [8, 2048, 1280], P(('rep', 'dp'))
- w_gate: bfloat16 [2, 1280, 4096], replicated
- w_up: bfloat16 [2, 1280, 4096], replicated
- w_down: bfloat16 [2, 4096, 1280], replicated
- m_w_gate: float32 [2, 1280, 4096], P(None, 'dp')
- m_w_up: float32 [2, 1280, 4096], P(None, 'dp')
- m_w_down: float32 [2, 4096, 1280], P(None, 'dp')
- v_w_gate: float32 [2, 1280, 4096], P(None, 'dp')
- v_w_up: float32 [2, 1280, 4096], P(None, 'dp')
- v_w_down: float32 [2, 4096, 1280], P(None, 'dp')
Outputs:
- output 1: bfloat16 [2, 1280, 4096], P('rep')
- output 2: bfloat16 [2, 1280, 4096], P('rep')
- output 3: bfloat16 [2, 4096, 1280], P('rep')
- output 4: float32 [2, 1280, 4096], P('rep', 'dp')
- output 5: float32 [2, 1280, 4096], P('rep', 'dp')
- output 6: float32 [2, 4096, 1280], P('rep', 'dp')
- output 7: float32 [2, 1280, 4096], P('rep', 'dp')
- output 8: float32 [2, 1280, 4096], P('rep', 'dp')
- output 9: float32 [2, 4096, 1280], P('rep', 'dp')
All inputs are finite; a program needn't handle non-finite values.
Results may differ from the reference program's by a relative error of at most 0.022.
Values are sent between devices in bfloat16 or wider.
A program may use at most 2 GiB of HBM per device.

```python
import jax
import jax.numpy as jnp
from jax import lax

SEQUENCES = 8
TOKENS = 2048
D = 1280
FF = 4096
LAYERS = 2
NAMES = ("w_gate", "w_up", "w_down")
SHAPES = {"w_gate": (LAYERS, D, FF), "w_up": (LAYERS, D, FF), "w_down": (LAYERS, FF, D)}


def bump(key, n, height):
    away = (jnp.arange(n, dtype=jnp.int32) - jax.random.randint(key, (), 0, n, jnp.int32)) % n
    return jnp.where(away < n // 8, height, 1.0)


def together(key, own, strength):
    shared = jax.random.normal(key, own.shape[1:], jnp.float32)
    return (own + strength * shared) * lax.rsqrt(1 + strength * strength)


def setup_inputs(seed: int = 0, part: int = 0) -> dict:
    kx, kdy, ka, kb, kz, kf, kh, kl, *keys = jax.random.split(jax.random.key(seed), 8 + 3 * len(NAMES))
    kx, kdy, ka, kb = (jax.random.fold_in(k, part) for k in (kx, kdy, ka, kb))
    kw, km, kv = (keys[i::3] for i in range(3))
    shape = (SEQUENCES, TOKENS, D)
    much_x, much_dy = jax.random.uniform(kz, (2,), jnp.float32, 0.0, 1.0)
    loud = 2.0 ** jax.random.uniform(jax.random.fold_in(kz, 1), (), jnp.float32, -1.0, 2.0)
    layers = 2.0 ** jax.random.uniform(kl, (LAYERS, 1, 1), jnp.float32, -1.0, 1.0)
    x = together(ka, jax.random.normal(kx, shape, jnp.float32), much_x) * bump(kf, D, 4.0)
    dy = together(kb, jax.random.normal(kdy, shape, jnp.float32), much_dy)
    drawn = {"x": x.astype(jnp.bfloat16), "dy": (loud * dy * (SEQUENCES * TOKENS) ** -0.5).astype(jnp.bfloat16)}
    for key, name in zip(kw, NAMES, strict=True):
        w = jax.random.normal(key, SHAPES[name], jnp.float32) * SHAPES[name][1] ** -0.5
        drawn[name] = (w * {"w_gate": 1.0, "w_up": bump(kh, FF, 4.0), "w_down": layers}[name]).astype(jnp.bfloat16)
    for key, name in zip(km, NAMES, strict=True):
        drawn[f"m_{name}"] = 0.1 * jax.random.normal(key, SHAPES[name], jnp.float32)
    for key, name in zip(kv, NAMES, strict=True):
        drawn[f"v_{name}"] = jax.random.uniform(key, SHAPES[name], jnp.float32, 0.005, 0.015)
    return drawn


def matmul(a, w):
    return jnp.dot(a, w, preferred_element_type=jnp.float32).astype(jnp.bfloat16)


def normed(h):
    wide = h.astype(jnp.float32)
    scale = lax.rsqrt(jnp.mean(wide**2, -1, keepdims=True) + 1e-6)
    return (wide * scale).astype(jnp.bfloat16)


def layer(h, w):
    a = normed(h)
    gate = jnp.dot(a, w["w_gate"], preferred_element_type=jnp.float32)
    up = jnp.dot(a, w["w_up"], preferred_element_type=jnp.float32)
    return h + matmul((jax.nn.silu(gate) * up).astype(jnp.bfloat16), w["w_down"])


def adamw(w, m, v, g):
    m = 0.9 * m + 0.1 * g
    v = 0.95 * v + 0.05 * g * g
    step = m * lax.rsqrt(v + 1e-8) + 0.1 * w
    return (w - 0.02 * step).astype(jnp.bfloat16), m, v


def stack(weights, h):
    return lax.scan(lambda h, w: (layer(h, w), None), h, weights)[0]


def reference(x, dy, w_gate, w_up, w_down, m_w_gate, m_w_up, m_w_down, v_w_gate, v_w_up, v_w_down):
    weights = dict(zip(NAMES, (w_gate, w_up, w_down), strict=True))

    def take(so_far, sequence):
        h, by_y = sequence
        _, back = jax.vjp(lambda w: stack(w, h), weights)
        return jax.tree.map(lambda total, term: total + term.astype(jnp.float32), so_far, back(by_y)[0]), None

    none_yet = {name: jnp.zeros(w.shape, jnp.float32) for name, w in weights.items()}
    by_weights, _ = lax.scan(take, none_yet, (x, dy))
    gradients = [by_weights[name].astype(jnp.bfloat16).astype(jnp.float32) for name in NAMES]
    new = [
        adamw(w.astype(jnp.float32), m, v, g)
        for w, m, v, g in zip((w_gate, w_up, w_down), (m_w_gate, m_w_up, m_w_down), (v_w_gate, v_w_up, v_w_down), gradients, strict=True)
    ]
    return tuple(one[which] for which in range(3) for one in new)
```

```python
import jax
import jax.numpy as jnp
from jax import lax
from jax.sharding import PartitionSpec as P

F32, BF16 = jnp.float32, jnp.bfloat16


def normed(h):
    wide = h.astype(F32)
    scale = lax.rsqrt(jnp.mean(wide**2, -1, keepdims=True) + 1e-6)
    return (wide * scale).astype(BF16)


def dot(a, b, dims):
    return lax.dot_general(a, b, (dims, ((), ())), preferred_element_type=F32)


NN, NT, TN = ((1,), (0,)), ((1,), (1,)), ((0,), (0,))


def up_part(a, wg, wu):
    gate = dot(a, wg, NN)
    up = dot(a, wu, NN)
    return gate, up, (jax.nn.silu(gate) * up).astype(BF16)


def through_product(gate, up, d):
    wide = d.astype(F32)
    s = jax.nn.sigmoid(gate)
    return (wide * up * (s * (1 + gate * (1 - s)))).astype(BF16), (wide * gate * s).astype(BF16)


def adamw(w, m, v, g):
    m = 0.9 * m + 0.1 * g
    v = 0.95 * v + 0.05 * g * g
    step = m * lax.rsqrt(v + 1e-8) + 0.1 * w
    return (w - 0.02 * step).astype(BF16), m, v


def solution(mesh):
    n = mesh.shape["dp"]

    def step(x, dy, w_gate, w_up, w_down, *moments):
        weights = (w_gate, w_up, w_down)
        x, dy = x[0], dy[0]
        me = lax.axis_index("dp")
        done = {}

        def scatter(term):
            return lax.psum_scatter(term.astype(BF16), "dp", scatter_dimension=0, tiled=True)

        def update(layer, which, g):
            w = weights[which][layer]
            rows = w.shape[0] // n
            own = lax.dynamic_slice_in_dim(w, me * rows, rows, 0).astype(F32)
            new, m, v = adamw(own, moments[which][layer], moments[3 + which][layer], g.astype(F32))
            done[layer, which] = lax.all_gather(new, "dp", axis=0, tiled=True), m, v

        a0 = normed(x)
        gate0, up0, act0 = up_part(a0, w_gate[0], w_up[0])
        h1 = x + dot(act0, w_down[0], NN).astype(BF16)
        a1, back1 = jax.vjp(normed, h1)
        gate1, up1, act1 = up_part(a1, w_gate[1], w_up[1])
        g_d1 = scatter(dot(act1, dy, TN))
        dact1 = dot(dy, w_down[1], NT).astype(BF16)
        dg1, du1 = through_product(gate1, up1, dact1)
        g_g1 = scatter(dot(a1, dg1, TN))
        g_u1 = scatter(dot(a1, du1, TN))
        da1 = dot(dg1, w_gate[1], NT).astype(BF16) + dot(du1, w_up[1], NT).astype(BF16)
        dh1 = dy + back1(da1)[0]
        g_d0 = scatter(dot(act0, dh1, TN))
        dact0 = dot(dh1, w_down[0], NT).astype(BF16)
        dg0, du0 = through_product(gate0, up0, dact0)
        g_g0 = scatter(dot(a0, dg0, TN))
        g_u0 = scatter(dot(a0, du0, TN))
        update(1, 2, g_d1)
        update(1, 0, g_g1)
        update(1, 1, g_u1)
        update(0, 2, g_d0)
        update(0, 0, g_g0)
        update(0, 1, g_u0)
        return tuple(jnp.stack([done[0, which][k], done[1, which][k]]) for k in range(3) for which in range(3))

    seq, whole, block, group = P(("rep", "dp"), None, None), P(None, None, None), P(None, "dp", None), P("rep", None, None)
    return jax.shard_map(
        step,
        mesh=mesh,
        in_specs=(seq, seq) + (whole,) * 3 + (block,) * 6,
        out_specs=(group,) * 3 + (P("rep", "dp", None),) * 6,
        check_vma=False,
    )
```

```python
import functools

import jax
import jax.numpy as jnp
from jax import lax
from jax.experimental import pallas as pl
from jax.experimental.pallas import tpu as pltpu
from jax.sharding import PartitionSpec as P

F32, BF16 = jnp.float32, jnp.bfloat16
MESH = pl.DeviceIdType.MESH
NN, NT, TN = ((1,), (0,)), ((1,), (1,)), ((0,), (0,))

TILE = 512
SEG = 128
OWNERS = 4


def normed(h):
    wide = h.astype(F32)
    scale = lax.rsqrt(jnp.mean(wide**2, -1, keepdims=True) + 1e-6)
    return (wide * scale).astype(BF16)


def dot(a, b, dims):
    return lax.dot_general(a, b, (dims, ((), ())), preferred_element_type=F32)


def adamw(w, m, v, g):
    m = 0.9 * m + 0.1 * g
    v = 0.95 * v + 0.05 * g * g
    step = m * lax.rsqrt(v + 1e-8) + 0.1 * w
    return (w - 0.02 * step).astype(BF16), m, v


def layer_kernel(layer, save, *refs):
    refs = list(refs)
    a, at, cot, wg, wu, wd = refs[:6]
    gg, gu, gd = refs[6:9]
    del refs[:9]
    if save:
        dgo, duo = refs[:2]
        del refs[:2]
    (a_v, at_v, cot_v, wg_v, wu_v, wd_v, act_v, dg_v, du_v, t0, t1) = refs[:11]
    del refs[:11]
    (dk, ds0, dr0, ds1, dr1, ds2, dr2) = refs[:7]
    del refs[:7]
    (k, s0, r0, s1, r1, s2, r2) = refs[:7]
    del refs[:7]
    (in_sem, at_sem, w_sem, save_sem, d_send, d_recv, send, recv, d_free, free) = refs

    tokens, width = a.shape
    hidden = wg.shape[2]
    block = SEG * OWNERS
    blocks = hidden // block
    part = hidden // (2 * OWNERS)
    rows = width // (2 * OWNERS)
    tiles = tokens // TILE
    temp = (t0, t1)

    me = lax.axis_index("dp")
    group = lax.axis_index("rep")
    x, y, c = me // 4, (me // 2) % 2, me % 2
    over_x, over_y = me + 4 - 8 * x, me + 2 - 4 * y
    peers = (me + 1 - 2 * c, (1 - c) * over_x + c * over_y, (1 - c) * over_y + c * over_x)
    first = (1 - c) * x + c * y
    second = (1 - c) * y + c * x

    def at_peer(stage):
        return (group, peers[stage])

    def columns(j, p):
        kind = j % 2
        swapped = (p % 2) * 2 + p // 2
        chip = p + kind * (swapped - p)
        return pl.multiple_of((2 * chip + kind) * part + (j // 2) * SEG, SEG)

    def load_weights(j):
        slot = j % 2
        for p in range(OWNERS):
            here = pl.ds(columns(j, p), SEG)
            there = pl.ds(p * SEG, SEG)
            pltpu.make_async_copy(wg.at[layer, :, here], wg_v.at[slot, :, there], w_sem.at[slot, 0]).start()
            pltpu.make_async_copy(wu.at[layer, :, here], wu_v.at[slot, :, there], w_sem.at[slot, 1]).start()
            pltpu.make_async_copy(wd.at[layer, here], wd_v.at[slot, there], w_sem.at[slot, 2]).start()

    def wait_weights(j):
        slot = j % 2
        for i, buffer in enumerate((wg_v, wu_v, wd_v)):
            pltpu.make_async_copy(buffer.at[slot], buffer.at[slot], w_sem.at[slot, i]).wait()

    def input_copies(i):
        here = pl.ds(i * TILE, TILE)
        return (
            pltpu.make_async_copy(a.at[here], a_v.at[here], in_sem.at[0, i]),
            pltpu.make_async_copy(cot.at[here], cot_v.at[here], in_sem.at[1, i]),
        )

    def save_copies(j):
        copies = []
        for p in range(OWNERS):
            here, there = pl.ds(columns(j, p), SEG), pl.ds(p * SEG, SEG)
            copies.append(pltpu.make_async_copy(dg_v.at[:, there], dgo.at[:, here], save_sem.at[0, p]))
            copies.append(pltpu.make_async_copy(du_v.at[:, there], duo.at[:, here], save_sem.at[1, p]))
        return copies

    load_weights(0)
    for i in range(tiles):
        for copy in input_copies(i):
            copy.start()
    at_copy = pltpu.make_async_copy(at, at_v, at_sem)
    at_copy.start()

    barrier = pltpu.get_barrier_semaphore()
    for stage in range(3):
        pl.semaphore_signal(barrier, inc=1, device_id=at_peer(stage), device_id_type=MESH)
    pl.semaphore_wait(barrier, 3)

    def project(i, slot):
        here = pl.ds(i * TILE, TILE)
        t = temp[i % 2]
        t[0] = dot(a_v[here], wg_v[slot], NN)
        t[1] = dot(a_v[here], wu_v[slot], NN)
        t[2] = dot(cot_v[here], wd_v[slot], NT)

    def through_product(i):
        here = pl.ds(i * TILE, TILE)
        t = temp[i % 2]
        gate, up = t[0], t[1]
        d = t[2].astype(BF16).astype(F32)
        s = 1.0 / (1.0 + jnp.exp(-gate))
        silu = gate * s
        act_v[here] = (silu * up).astype(BF16)
        du_v[here] = (d * silu).astype(BF16)
        dg_v[here] = (d * up * (s + silu * (1.0 - s))).astype(BF16)

    half, quarter = block // 2, block // 4
    d_first = pl.multiple_of(first * half, half)
    d_away = pl.multiple_of((1 - first) * half, half)
    d_second = pl.multiple_of(second * quarter, quarter)
    d_other = pl.multiple_of((1 - second) * quarter, quarter)

    def d_copy(stage):
        source, target = ((ds0, dr0), (ds1, dr1), (ds2, dr2))[stage]
        return pltpu.make_async_remote_copy(
            source, target, d_send.at[stage], d_recv.at[stage], device_id=at_peer(stage), device_id_type=MESH
        )

    def d_start(j, stage):
        @pl.when(j >= 2)
        def _():
            pl.semaphore_wait(d_free.at[stage], 1)

        d_copy(stage).start()

    def d_term(j):
        dk[...] = dot(act_v[...], cot_v[...], TN)

        @pl.when(j % 2 != c)
        def _():
            ds0[...] = dk[...].astype(BF16)
            d_start(j, 0)

    def d_one(j):
        @pl.when(j % 2 != c)
        def _():
            d_copy(0).wait_send()

        @pl.when(j % 2 == c)
        def _():
            d_copy(0).wait_recv()
            here = pl.ds(d_away, half)
            ds1[...] = (dk[here] + dr0[here].astype(F32)).astype(BF16)
            d_start(j, 1)

    def d_two(j):
        @pl.when(j % 2 == c)
        def _():
            d_copy(1).wait()
            here = pl.ds(pl.multiple_of(d_first + d_other, quarter), quarter)
            ds2[...] = (dk[here] + dr0[here].astype(F32) + dr1[pl.ds(d_other, quarter)].astype(F32)).astype(BF16)
            d_start(j, 2)

    def d_three(j):
        @pl.when(j % 2 == c)
        def _():
            d_copy(2).wait()
            here = pl.ds(pl.multiple_of(d_first + d_second, quarter), quarter)
            total = dk[here] + dr0[here].astype(F32) + dr1[pl.ds(d_second, quarter)].astype(F32) + dr2[...].astype(F32)
            gd[pl.ds(pl.multiple_of((j // 2) * SEG, SEG), SEG)] = total.astype(BF16)

            @pl.when(j + 2 < blocks)
            def _():
                for stage in range(3):
                    pl.semaphore_signal(d_free.at[stage], inc=1, device_id=at_peer(stage), device_id_type=MESH)

    first_rows = pl.multiple_of(first * 2 * rows, 2 * rows)
    away_rows = pl.multiple_of((1 - first) * 2 * rows, 2 * rows)
    second_rows = pl.multiple_of(second * rows, rows)
    other_rows = pl.multiple_of((1 - second) * rows, rows)

    def copy_of(j, w, stage):
        slot = j % 2
        source, target = ((s0, r0), (s1, r1), (s2, r2))[stage]
        return pltpu.make_async_remote_copy(
            source.at[w, slot],
            target.at[w, slot],
            send.at[w, slot, stage],
            recv.at[w, slot, stage],
            device_id=at_peer(stage),
            device_id_type=MESH,
        )

    def start(j, w, stage):
        @pl.when(j >= 2)
        def _():
            pl.semaphore_wait(free.at[w, stage], 1)

        copy_of(j, w, stage).start()

    def term_away(j, w):
        s0[w, j % 2] = dot(at_v[1 - c], (dg_v, du_v)[w][...], NN).astype(BF16)
        start(j, w, 0)

    def term_kept(j, w):
        k[w, j % 2] = dot(at_v[c], (dg_v, du_v)[w][...], NN)

    def one(j, w):
        slot = j % 2
        copy_of(j, w, 0).wait()
        here = pl.ds(away_rows, 2 * rows)
        s1[w, slot] = (k[w, slot, here] + r0[w, slot, here].astype(F32)).astype(BF16)
        start(j, w, 1)

    def two(j, w):
        slot = j % 2
        copy_of(j, w, 1).wait()
        here = pl.ds(pl.multiple_of(first_rows + other_rows, rows), rows)
        s2[w, slot] = (
            k[w, slot, here] + r0[w, slot, here].astype(F32) + r1[w, slot, pl.ds(other_rows, rows)].astype(F32)
        ).astype(BF16)
        start(j, w, 2)

    def three(j, w):
        slot = j % 2
        copy_of(j, w, 2).wait()
        here = pl.ds(pl.multiple_of(first_rows + second_rows, rows), rows)
        there = pl.ds(second_rows, rows)
        for p in range(OWNERS):
            at_p = pl.ds(p * SEG, SEG)
            total = (
                k[w, slot, here, at_p]
                + r0[w, slot, here, at_p].astype(F32)
                + r1[w, slot, there, at_p].astype(F32)
                + r2[w, slot, :, at_p].astype(F32)
            )
            (gg, gu)[w][:, pl.ds(columns(j, p), SEG)] = total.astype(BF16)

        @pl.when(j + 2 < blocks)
        def _():
            for stage in range(3):
                pl.semaphore_signal(free.at[w, stage], inc=1, device_id=at_peer(stage), device_id_type=MESH)

    late = (
        lambda j: one(j, 1),
        d_two,
        lambda j: two(j, 0),
        d_three,
        lambda j: two(j, 1),
        lambda j: three(j, 0),
        lambda j: three(j, 1),
    )

    def step(j, carry):
        def after(n):
            @pl.when(j >= 1)
            def _():
                late[n](j - 1)

        slot = j % 2

        @pl.when(j + 1 < blocks)
        def _():
            load_weights(j + 1)

        wait_weights(j)
        for i in range(tiles):

            @pl.when(j == 0)
            def _():
                for copy in input_copies(i):
                    copy.wait()

            if save and i == 1:

                @pl.when(j >= 1)
                def _():
                    for copy in save_copies(j - 1):
                        copy.wait()

            project(i, slot)
            if i >= 1:
                through_product(i - 1)
            if i < 4:
                after(i)
        through_product(tiles - 1)
        after(4)
        if save:
            for copy in save_copies(j):
                copy.start()

        @pl.when(j == 0)
        def _():
            at_copy.wait()

        d_term(j)
        after(5)
        term_away(j, 0)
        after(6)
        term_kept(j, 0)
        d_one(j)
        term_away(j, 1)
        one(j, 0)
        term_kept(j, 1)
        return carry

    lax.fori_loop(0, blocks, step, 0)
    for event in late:
        event(blocks - 1)
    if save:
        for copy in save_copies(blocks - 1):
            copy.wait()


def layer_gradients(layer, save, a, at, cot, wg, wu, wd):
    tokens, width = a.shape
    hidden = wg.shape[2]
    block = SEG * OWNERS
    rows, part = width // (2 * OWNERS), hidden // (2 * OWNERS)
    half, quarter = block // 2, block // 4
    anywhere, vmem = pl.BlockSpec(memory_space=pl.ANY), pl.BlockSpec(memory_space=pltpu.VMEM)
    out_shape = [
        jax.ShapeDtypeStruct((rows, hidden), BF16),
        jax.ShapeDtypeStruct((rows, hidden), BF16),
        jax.ShapeDtypeStruct((part, width), BF16),
    ]
    out_specs = [vmem] * 3
    if save:
        out_shape += [jax.ShapeDtypeStruct((tokens, hidden), BF16)] * 2
        out_specs += [anywhere] * 2
    dma, regular = pltpu.SemaphoreType.DMA, pltpu.SemaphoreType.REGULAR
    return pl.pallas_call(
        functools.partial(layer_kernel, layer, save),
        name=f"layer_{layer}",
        out_shape=out_shape,
        in_specs=[anywhere] * 6,
        out_specs=out_specs,
        scratch_shapes=[
            pltpu.VMEM((tokens, width), BF16),
            pltpu.VMEM((2, width // 2, tokens), BF16),
            pltpu.VMEM((tokens, width), BF16),
            pltpu.VMEM((2, width, block), BF16),
            pltpu.VMEM((2, width, block), BF16),
            pltpu.VMEM((2, block, width), BF16),
            pltpu.VMEM((tokens, block), BF16),
            pltpu.VMEM((tokens, block), BF16),
            pltpu.VMEM((tokens, block), BF16),
            pltpu.VMEM((3, TILE, block), F32),
            pltpu.VMEM((3, TILE, block), F32),
            pltpu.VMEM((block, width), F32),
            pltpu.VMEM((block, width), BF16),
            pltpu.VMEM((block, width), BF16),
            pltpu.VMEM((half, width), BF16),
            pltpu.VMEM((half, width), BF16),
            pltpu.VMEM((quarter, width), BF16),
            pltpu.VMEM((quarter, width), BF16),
            pltpu.VMEM((2, 2, 4 * rows, block), F32),
            pltpu.VMEM((2, 2, 4 * rows, block), BF16),
            pltpu.VMEM((2, 2, 4 * rows, block), BF16),
            pltpu.VMEM((2, 2, 2 * rows, block), BF16),
            pltpu.VMEM((2, 2, 2 * rows, block), BF16),
            pltpu.VMEM((2, 2, rows, block), BF16),
            pltpu.VMEM((2, 2, rows, block), BF16),
            dma((2, tokens // TILE)),
            dma,
            dma((2, 3)),
            dma((2, OWNERS)),
            dma((3,)),
            dma((3,)),
            dma((2, 2, 3)),
            dma((2, 2, 3)),
            regular((3,)),
            regular((2, 3)),
        ],
        compiler_params=pltpu.CompilerParams(
            collective_id=layer, has_side_effects=True, vmem_limit_bytes=67043328
        ),
        cost_estimate=pl.CostEstimate(
            flops=12 * tokens * width * hidden, bytes_accessed=10 * width * hidden, transcendentals=tokens * hidden
        ),
    )(a, at, cot, wg, wu, wd)


def place_kernel(layer, parts, *refs):
    sources, (out, buffer, read, write) = refs[: len(parts)], refs[-4:]
    me = lax.axis_index("dp")
    x, y, c = me // 4, (me // 2) % 2, me % 2
    copies = []
    for source, (blocks, index, other) in zip(sources, parts, strict=True):
        core = 1 - c if other else c
        rows = source.shape[0] // blocks
        for i in range(blocks):
            second, first = (index + i) % 2, (index + i) // 2
            x_flip, y_flip = core * second + (1 - core) * first, core * first + (1 - core) * second
            owner = 4 * (x + x_flip - 2 * x * x_flip) + 2 * (y + y_flip - 2 * y * y_flip) + core
            there = pl.multiple_of(owner * rows, 16)
            n = len(copies)
            copies.append(
                (
                    pltpu.make_async_copy(source.at[pl.ds(i * rows, rows)], buffer.at[n], read.at[n]),
                    pltpu.make_async_copy(buffer.at[n], out.at[layer, pl.ds(there, rows)], write.at[n]),
                )
            )
    for first, _ in copies:
        first.start()
    for first, second in copies:
        first.wait()
        second.start()
    for _, second in copies:
        second.wait()


def place(out, layer, *pieces):
    sources, parts = [p[0] for p in pieces], tuple(p[1:] for p in pieces)
    rows, columns = sources[0].shape[0] // parts[0][0], sources[0].shape[1]
    count = sum(p[0] for p in parts)
    anywhere = pl.BlockSpec(memory_space=pl.ANY)
    if out is not None:
        sources.append(out)
    return pl.pallas_call(
        functools.partial(place_kernel, layer, parts),
        name=f"place_{layer}",
        out_shape=jax.ShapeDtypeStruct((2, 8 * rows, columns), BF16),
        in_specs=[anywhere] * len(sources),
        out_specs=anywhere,
        input_output_aliases={} if out is None else {len(parts): 0},
        scratch_shapes=[
            pltpu.VMEM((count, rows, columns), BF16),
            pltpu.SemaphoreType.DMA((count,)),
            pltpu.SemaphoreType.DMA((count,)),
        ],
        compiler_params=pltpu.CompilerParams(vmem_limit_bytes=16 << 20),
        cost_estimate=pl.CostEstimate(flops=count * rows * columns * 1000, bytes_accessed=4 * count * rows * columns, transcendentals=0),
    )(*sources)


def moments_kernel(m, v, g0, g1, new_m, new_v):
    first = pl.program_id(0) == 0
    g = jnp.where(first, g0[...], g1[...]).astype(F32)
    new_m[0] = 0.9 * m[0] + 0.1 * g
    new_v[0] = 0.95 * v[0] + 0.05 * g * g


def moments_of(m, v, g0, g1):
    layers, rows, columns = m.shape
    count = rows // 4 if rows % 64 == 0 else rows // 5
    wide = pl.BlockSpec((1, count, columns), lambda layer, i: (layer, i, 0))
    narrow = pl.BlockSpec((count, columns), lambda layer, i: (i, 0))
    return pl.pallas_call(
        moments_kernel,
        name="moments",
        grid=(layers, rows // count),
        out_shape=[jax.ShapeDtypeStruct(m.shape, F32)] * 2,
        in_specs=[wide, wide, narrow, narrow],
        out_specs=[wide, wide],
        compiler_params=pltpu.CompilerParams(vmem_limit_bytes=24 << 20),
        cost_estimate=pl.CostEstimate(flops=m.size * 500, bytes_accessed=18 * m.size, transcendentals=0),
    )(m, v, g0, g1)


def solution(mesh):
    n = mesh.shape["dp"]

    def pairs(on_core_0, on_core_1):
        return [(i, i ^ (on_core_1 if i % 2 else on_core_0)) for i in range(n)]

    to_second, to_first, to_core = pairs(2, 4), pairs(4, 2), pairs(1, 1)

    def step(x, dy, w_gate, w_up, w_down, *moments):
        weights = (w_gate, w_up, w_down)
        x, dy = x[0], dy[0]
        me = lax.axis_index("dp")

        def turned(a):
            tokens, width = a.shape
            t = a.T.reshape(2, 2, 2, width // 8, tokens)
            return jnp.stack([t[:, :, 0], t[:, :, 1].swapaxes(0, 1)]).reshape(2, width // 2, tokens)

        def new_weight(layer, which, g):
            w = weights[which]
            rows = w.shape[1] // n
            own = lax.dynamic_slice(w, (layer, me * rows, 0), (1, rows, w.shape[2]))[0].astype(F32)
            return adamw(own, moments[which][layer], moments[3 + which][layer], g.astype(F32))[0]

        def wait_for(*arrays):
            return lax.optimization_barrier(arrays)

        def send(array, to):
            return lax.ppermute(array, "dp", to)

        a0 = normed(x)
        gate, up = dot(a0, w_gate[0], NN), dot(a0, w_up[0], NN)
        h1 = x + dot((jax.nn.silu(gate) * up).astype(BF16), w_down[0], NN).astype(BF16)
        a1, back1 = jax.vjp(normed, h1)
        gg1, gu1, gd1, dg, du = layer_gradients(1, True, a1, turned(a1), dy, *weights)
        own1 = [new_weight(1, which, g) for which, g in ((0, gg1), (1, gu1), (2, gd1))]
        dg, du, *own1 = wait_for(dg, du, *own1)
        got1 = [send(own, to_second) for own in own1]
        da1 = dot(dg, w_gate[1], NT).astype(BF16) + dot(du, w_up[1], NT).astype(BF16)
        dh1 = dy + back1(da1)[0]
        dh1, *got1 = wait_for(dh1, *got1)
        two1 = [jnp.concatenate([own, got]) for own, got in zip(own1, got1)]
        more1 = [send(two, to_first) for two in two1]
        gg0, gu0, gd0 = layer_gradients(0, False, a0, turned(a0), dh1, *weights)
        gg0, gu0, gd0, *more1 = wait_for(gg0, gu0, gd0, *more1)
        own0 = [new_weight(0, which, g) for which, g in ((0, gg0), (1, gu0), (2, gd0))]
        gg0, gu0, gd0, own0[0], own0[1], own0[2], *more1 = wait_for(gg0, gu0, gd0, *own0, *more1)
        got0 = [send(own, to_second) for own in own0]
        new = [moments_of(moments[i], moments[3 + i], *g) for i, g in enumerate(((gg0, gg1), (gu0, gu1), (gd0, gd1)))]
        out = [place(None, 1, (two, 2, 0, False), (more, 2, 2, False)) for two, more in zip(two1, more1)]
        got0[0], *done = wait_for(got0[0], *(array for pair in new for array in pair))
        new = [tuple(done[i : i + 2]) for i in (0, 2, 4)]
        other1 = [(send(two, to_core), send(more, to_core)) for two, more in zip(two1, more1)]
        two0, more0 = [None] * 3, [None] * 3
        for i in range(3):
            if i:
                got0[i], out[i - 1] = wait_for(got0[i], out[i - 1])
            two0[i] = jnp.concatenate([own0[i], got0[i]])
            more0[i] = send(two0[i], to_first)
        for i in range(3):
            (two, more), there = other1[i], send(two0[i], to_core)
            out[i] = place(out[i], 1, (two, 2, 0, True), (more, 2, 2, True))
            out[i] = place(out[i], 0, (two0[i], 2, 0, False), (there, 2, 0, True))
            more0[i], out[i] = wait_for(more0[i], out[i])
            out[i] = place(out[i], 0, (more0[i], 2, 2, False), (send(more0[i], to_core), 2, 2, True))
        return (*out, *(m for m, _ in new), *(v for _, v in new))

    seq, whole, block, group = P(("rep", "dp"), None, None), P(None, None, None), P(None, "dp", None), P("rep", None, None)
    return jax.shard_map(
        step,
        mesh=mesh,
        in_specs=(seq, seq) + (whole,) * 3 + (block,) * 6,
        out_specs=(group,) * 3 + (P("rep", "dp", None),) * 6,
        check_vma=False,
    )
```

```python
import functools

import jax
import jax.numpy as jnp
from jax import lax
from jax.experimental import pallas as pl
from jax.experimental.pallas import tpu as pltpu
from jax.sharding import PartitionSpec as P

F32, BF16 = jnp.float32, jnp.bfloat16
MESH = pl.DeviceIdType.MESH
NN, NT, TN = ((1,), (0,)), ((1,), (1,)), ((0,), (0,))

TILE = 512
SEG = 128
OWNERS = 4
CHUNK = 16


def dot(a, b, dims):
    return lax.dot_general(a, b, (dims, ((), ())), preferred_element_type=F32)


def adamw(w, m, v, g):
    m = 0.9 * m + 0.1 * g
    v = 0.95 * v + 0.05 * g * g
    step = m * lax.rsqrt(v + 1e-8) + 0.1 * w
    return (w - 0.02 * step).astype(BF16), m, v


def layer_kernel(layer, save, *refs):
    refs = list(refs)
    a, cot, wg, wu, wd = refs[:5]
    gg, gu, gd = refs[5:8]
    del refs[:8]
    if save:
        dgo, duo = refs[:2]
        del refs[:2]
    (a_v, at_v, cot_v, wg_v, wu_v, wd_v, act_v, dg_v, du_v, t0, t1) = refs[:11]
    del refs[:11]
    (dk, ds0, dr0, ds1, dr1, ds2, dr2) = refs[:7]
    del refs[:7]
    (k, s0, r0, s1, r1, s2, r2) = refs[:7]
    del refs[:7]
    (in_sem, w_sem, save_sem, d_send, d_recv, send, recv, d_free, free) = refs

    tokens, width = a.shape
    hidden = wg.shape[2]
    block = SEG * OWNERS
    blocks = hidden // block
    part = hidden // (2 * OWNERS)
    rows = width // (2 * OWNERS)
    tiles = tokens // TILE
    temp = (t0, t1)

    me = lax.axis_index("dp")
    group = lax.axis_index("rep")
    x, y, c = me // 4, (me // 2) % 2, me % 2
    over_x, over_y = me + 4 - 8 * x, me + 2 - 4 * y
    peers = (me + 1 - 2 * c, (1 - c) * over_x + c * over_y, (1 - c) * over_y + c * over_x)
    first = (1 - c) * x + c * y
    second = (1 - c) * y + c * x

    def at_peer(stage):
        return (group, peers[stage])

    def columns(j, p):
        kind = j % 2
        swapped = (p % 2) * 2 + p // 2
        chip = p + kind * (swapped - p)
        return pl.multiple_of((2 * chip + kind) * part + (j // 2) * SEG, SEG)

    def load_weights(j):
        for p in range(OWNERS):
            here = pl.ds(columns(j, p), SEG)
            there = pl.ds(p * SEG, SEG)
            pltpu.make_async_copy(wg.at[layer, :, here], wg_v.at[:, there], w_sem.at[0]).start()
            pltpu.make_async_copy(wu.at[layer, :, here], wu_v.at[:, there], w_sem.at[1]).start()
            pltpu.make_async_copy(wd.at[layer, here], wd_v.at[there], w_sem.at[2]).start()

    def wait_weights():
        for i, buffer in enumerate((wg_v, wu_v, wd_v)):
            pltpu.make_async_copy(buffer, buffer, w_sem.at[i]).wait()

    def input_copies(i):
        here = pl.ds(i * TILE, TILE)
        return (
            pltpu.make_async_copy(a.at[here], a_v.at[here], in_sem.at[0, i]),
            pltpu.make_async_copy(cot.at[here], cot_v.at[here], in_sem.at[1, i]),
        )

    def save_copies(j):
        copies = []
        for p in range(OWNERS):
            here, there = pl.ds(columns(j, p), SEG), pl.ds(p * SEG, SEG)
            copies.append(pltpu.make_async_copy(dg_v.at[:, there], dgo.at[:, here], save_sem.at[0, p]))
            copies.append(pltpu.make_async_copy(du_v.at[:, there], duo.at[:, here], save_sem.at[1, p]))
        return copies

    load_weights(0)
    for i in range(tiles):
        for copy in input_copies(i):
            copy.start()

    barrier = pltpu.get_barrier_semaphore()
    for stage in range(3):
        pl.semaphore_signal(barrier, inc=1, device_id=at_peer(stage), device_id_type=MESH)
    pl.semaphore_wait(barrier, 3)

    def turn(i):
        here = pl.ds(i * TILE, TILE)
        turned = a_v[here].T
        for o in range(2 * OWNERS):
            place = (o // 4) * 2 + (o // 2) % 2 if o % 2 == 0 else (o // 2) % 2 * 2 + o // 4
            at_v[o % 2, place * rows : (place + 1) * rows, here] = turned[o * rows : (o + 1) * rows]

    def project(i):
        here = pl.ds(i * TILE, TILE)
        t = temp[i % 2]
        t[0] = dot(a_v[here], wg_v[...], NN)
        t[1] = dot(a_v[here], wu_v[...], NN)
        t[2] = dot(cot_v[here], wd_v[...], NT)

    def through_product(i):
        t = temp[i % 2]
        for r in range(0, TILE, CHUNK):
            here = pl.ds(r, CHUNK)
            there = pl.ds(i * TILE + r, CHUNK)
            gate, up = t[0, here], t[1, here]
            d = t[2, here].astype(BF16).astype(F32)
            s = 1.0 / (1.0 + jnp.exp(-gate))
            silu = gate * s
            act_v[there] = (silu * up).astype(BF16)
            du_v[there] = (d * silu).astype(BF16)
            dg_v[there] = (d * up * (s + silu * (1.0 - s))).astype(BF16)

    half, quarter = block // 2, block // 4
    d_first = pl.multiple_of(first * half, half)
    d_away = pl.multiple_of((1 - first) * half, half)
    d_second = pl.multiple_of(second * quarter, quarter)
    d_other = pl.multiple_of((1 - second) * quarter, quarter)

    def d_copy(stage):
        source, target = ((ds0, dr0), (ds1, dr1), (ds2, dr2))[stage]
        return pltpu.make_async_remote_copy(
            source, target, d_send.at[stage], d_recv.at[stage], device_id=at_peer(stage), device_id_type=MESH
        )

    def d_start(j, stage):
        @pl.when(j >= 2)
        def _():
            pl.semaphore_wait(d_free.at[stage], 1)

        d_copy(stage).start()

    def d_term(j):
        dk[j % 2] = dot(act_v[...], cot_v[...], TN)

        @pl.when(j % 2 != c)
        def _():
            ds0[...] = dk[j % 2].astype(BF16)
            d_start(j, 0)

    def d_one(j):
        @pl.when(j % 2 != c)
        def _():
            d_copy(0).wait_send()

        @pl.when(j % 2 == c)
        def _():
            d_copy(0).wait_recv()
            here = pl.ds(d_away, half)
            ds1[...] = (dk[c, here] + dr0[here].astype(F32)).astype(BF16)
            d_start(j, 1)

    def d_two(j):
        @pl.when(j % 2 == c)
        def _():
            d_copy(1).wait()
            here = pl.ds(pl.multiple_of(d_first + d_other, quarter), quarter)
            ds2[...] = (dk[c, here] + dr0[here].astype(F32) + dr1[pl.ds(d_other, quarter)].astype(F32)).astype(BF16)
            d_start(j, 2)

    def d_three(j):
        @pl.when(j % 2 == c)
        def _():
            d_copy(2).wait()
            here = pl.ds(pl.multiple_of(d_first + d_second, quarter), quarter)
            total = dk[c, here] + dr0[here].astype(F32) + dr1[pl.ds(d_second, quarter)].astype(F32) + dr2[...].astype(F32)
            gd[pl.ds(pl.multiple_of((j // 2) * SEG, SEG), SEG)] = total.astype(BF16)

            @pl.when(j + 2 < blocks)
            def _():
                for stage in range(3):
                    pl.semaphore_signal(d_free.at[stage], inc=1, device_id=at_peer(stage), device_id_type=MESH)

    first_rows = pl.multiple_of(first * 2 * rows, 2 * rows)
    away_rows = pl.multiple_of((1 - first) * 2 * rows, 2 * rows)
    second_rows = pl.multiple_of(second * rows, rows)
    other_rows = pl.multiple_of((1 - second) * rows, rows)

    def copy_of(j, w, stage):
        slot = j % 2
        source, target = ((s0, r0), (s1, r1), (s2, r2))[stage]
        return pltpu.make_async_remote_copy(
            source.at[w, slot],
            target.at[w, slot],
            send.at[w, slot, stage],
            recv.at[w, slot, stage],
            device_id=at_peer(stage),
            device_id_type=MESH,
        )

    def start(j, w, stage):
        @pl.when(j >= 2)
        def _():
            pl.semaphore_wait(free.at[w, stage], 1)

        copy_of(j, w, stage).start()

    def term_away(j, w):
        s0[w, j % 2] = dot(at_v[1 - c], (dg_v, du_v)[w][...], NN).astype(BF16)
        start(j, w, 0)

    def term_kept(j, w):
        k[w, j % 2] = dot(at_v[c], (dg_v, du_v)[w][...], NN)

    def one(j, w):
        slot = j % 2
        copy_of(j, w, 0).wait()
        here = pl.ds(away_rows, 2 * rows)
        s1[w, slot] = (k[w, slot, here] + r0[w, slot, here].astype(F32)).astype(BF16)
        start(j, w, 1)

    def two(j, w):
        slot = j % 2
        copy_of(j, w, 1).wait()
        here = pl.ds(pl.multiple_of(first_rows + other_rows, rows), rows)
        s2[w, slot] = (
            k[w, slot, here] + r0[w, slot, here].astype(F32) + r1[w, slot, pl.ds(other_rows, rows)].astype(F32)
        ).astype(BF16)
        start(j, w, 2)

    def three(j, w):
        slot = j % 2
        copy_of(j, w, 2).wait()
        here = pl.ds(pl.multiple_of(first_rows + second_rows, rows), rows)
        there = pl.ds(second_rows, rows)
        for p in range(OWNERS):
            at_p = pl.ds(p * SEG, SEG)
            total = (
                k[w, slot, here, at_p]
                + r0[w, slot, here, at_p].astype(F32)
                + r1[w, slot, there, at_p].astype(F32)
                + r2[w, slot, :, at_p].astype(F32)
            )
            (gg, gu)[w][:, pl.ds(columns(j, p), SEG)] = total.astype(BF16)

        @pl.when(j + 2 < blocks)
        def _():
            for stage in range(3):
                pl.semaphore_signal(free.at[w, stage], inc=1, device_id=at_peer(stage), device_id_type=MESH)

    g, u = 0, 1

    def step(j, carry):
        def after(event, back, *args):
            @pl.when(j >= back)
            def _():
                event(j - back, *args)

        wait_weights()
        for i in range(tiles):

            @pl.when(j == 0)
            def _():
                for copy in input_copies(i):
                    copy.wait()
                turn(i)

            if save and i == 1:

                @pl.when(j >= 1)
                def _():
                    for copy in save_copies(j - 1):
                        copy.wait()

            project(i)
            if i >= 1:
                through_product(i - 1)
            if i == 0:
                after(one, 1, u)
                after(three, 2, g)
            if i == 1:
                after(three, 2, u)
            if i == tiles - 1:
                after(d_two, 1)

        @pl.when(j + 1 < blocks)
        def _():
            load_weights(j + 1)

        through_product(tiles - 1)
        if save:
            for copy in save_copies(j):
                copy.start()

        d_term(j)
        after(two, 1, g)
        term_away(j, g)
        term_kept(j, g)
        after(two, 1, u)
        d_one(j)
        term_away(j, u)
        one(j, g)
        after(d_three, 1)
        term_kept(j, u)
        return carry

    lax.fori_loop(0, blocks, step, 0)
    last = blocks - 1
    one(last, u)
    three(last - 1, g)
    three(last - 1, u)
    d_two(last)
    two(last, g)
    two(last, u)
    d_three(last)
    three(last, g)
    three(last, u)
    if save:
        for copy in save_copies(last):
            copy.wait()


def layer_gradients(layer, save, a, cot, wg, wu, wd):
    tokens, width = a.shape
    hidden = wg.shape[2]
    block = SEG * OWNERS
    rows, part = width // (2 * OWNERS), hidden // (2 * OWNERS)
    half, quarter = block // 2, block // 4
    anywhere, vmem = pl.BlockSpec(memory_space=pl.ANY), pl.BlockSpec(memory_space=pltpu.VMEM)
    out_shape = [
        jax.ShapeDtypeStruct((rows, hidden), BF16),
        jax.ShapeDtypeStruct((rows, hidden), BF16),
        jax.ShapeDtypeStruct((part, width), BF16),
    ]
    out_specs = [vmem] * 3
    if save:
        out_shape += [jax.ShapeDtypeStruct((tokens, hidden), BF16)] * 2
        out_specs += [anywhere] * 2
    dma, regular = pltpu.SemaphoreType.DMA, pltpu.SemaphoreType.REGULAR
    return pl.pallas_call(
        functools.partial(layer_kernel, layer, save),
        name=f"layer_{layer}",
        out_shape=out_shape,
        in_specs=[anywhere] * 5,
        out_specs=out_specs,
        scratch_shapes=[
            pltpu.VMEM((tokens, width), BF16),
            pltpu.VMEM((2, width // 2, tokens), BF16),
            pltpu.VMEM((tokens, width), BF16),
            pltpu.VMEM((width, block), BF16),
            pltpu.VMEM((width, block), BF16),
            pltpu.VMEM((block, width), BF16),
            pltpu.VMEM((tokens, block), BF16),
            pltpu.VMEM((tokens, block), BF16),
            pltpu.VMEM((tokens, block), BF16),
            pltpu.VMEM((3, TILE, block), F32),
            pltpu.VMEM((3, TILE, block), F32),
            pltpu.VMEM((2, block, width), F32),
            pltpu.VMEM((block, width), BF16),
            pltpu.VMEM((block, width), BF16),
            pltpu.VMEM((half, width), BF16),
            pltpu.VMEM((half, width), BF16),
            pltpu.VMEM((quarter, width), BF16),
            pltpu.VMEM((quarter, width), BF16),
            pltpu.VMEM((2, 2, 4 * rows, block), F32),
            pltpu.VMEM((2, 2, 4 * rows, block), BF16),
            pltpu.VMEM((2, 2, 4 * rows, block), BF16),
            pltpu.VMEM((2, 2, 2 * rows, block), BF16),
            pltpu.VMEM((2, 2, 2 * rows, block), BF16),
            pltpu.VMEM((2, 2, rows, block), BF16),
            pltpu.VMEM((2, 2, rows, block), BF16),
            dma((2, tokens // TILE)),
            dma((3,)),
            dma((2, OWNERS)),
            dma((3,)),
            dma((3,)),
            dma((2, 2, 3)),
            dma((2, 2, 3)),
            regular((3,)),
            regular((2, 3)),
        ],
        compiler_params=pltpu.CompilerParams(
            collective_id=layer, has_side_effects=True, vmem_limit_bytes=67043328
        ),
        cost_estimate=pl.CostEstimate(
            flops=12 * tokens * width * hidden, bytes_accessed=10 * width * hidden, transcendentals=tokens * hidden
        ),
    )(a, cot, wg, wu, wd)


def rows_of(ref, body):
    def step(i, carry):
        body(pl.ds(pl.multiple_of(i * CHUNK, CHUNK), CHUNK))
        return carry

    lax.fori_loop(0, ref.shape[0] // CHUNK, step, 0, unroll=4)


def scale_of(wide):
    return lax.rsqrt(jnp.mean(wide * wide, -1, keepdims=True) + 1e-6)


def forward_kernel(x, wg, wu, wd, a0, h1, a1, total, act, t0, t1):
    j = pl.program_id(0)
    temp = (t0, t1)
    tiles = x.shape[0] // TILE

    @pl.when(j == 0)
    def _():
        def start(here):
            wide = x[here].astype(F32)
            a0[here] = (wide * scale_of(wide)).astype(BF16)
            total[here] = jnp.zeros_like(wide)

        rows_of(x, start)

    def product(i):
        for r in range(0, TILE, CHUNK):
            gate, up = temp[i % 2][0, pl.ds(r, CHUNK)], temp[i % 2][1, pl.ds(r, CHUNK)]
            s = 1.0 / (1.0 + jnp.exp(-gate))
            act[i % 2, pl.ds(r, CHUNK)] = (gate * s * up).astype(BF16)

    def down(i):
        total[pl.ds(i * TILE, TILE)] += dot(act[i % 2], wd[0], NN)

    for i in range(tiles):
        here = pl.ds(i * TILE, TILE)
        temp[i % 2][0] = dot(a0[here], wg[0], NN)
        temp[i % 2][1] = dot(a0[here], wu[0], NN)
        if i >= 1:
            product(i - 1)
        if i >= 2:
            down(i - 2)
    product(tiles - 1)
    down(tiles - 2)
    down(tiles - 1)

    @pl.when(j == pl.num_programs(0) - 1)
    def _():
        def finish(here):
            h = x[here] + total[here].astype(BF16)
            h1[here] = h
            wide = h.astype(F32)
            a1[here] = (wide * scale_of(wide)).astype(BF16)

        rows_of(x, finish)


def forward(layer, x, wg, wu, wd):
    tokens, width = x.shape
    hidden = wg.shape[2]
    block = SEG * OWNERS
    whole = pl.BlockSpec(memory_space=pltpu.VMEM)
    across = pl.BlockSpec((1, width, block), lambda j: (layer, 0, j))
    return pl.pallas_call(
        forward_kernel,
        name="forward",
        grid=(hidden // block,),
        out_shape=[jax.ShapeDtypeStruct((tokens, width), BF16)] * 3,
        in_specs=[whole, across, across, pl.BlockSpec((1, block, width), lambda j: (layer, j, 0))],
        out_specs=[whole] * 3,
        scratch_shapes=[
            pltpu.VMEM((tokens, width), F32),
            pltpu.VMEM((2, TILE, block), BF16),
            pltpu.VMEM((2, TILE, block), F32),
            pltpu.VMEM((2, TILE, block), F32),
        ],
        compiler_params=pltpu.CompilerParams(vmem_limit_bytes=67043328),
        cost_estimate=pl.CostEstimate(
            flops=6 * tokens * width * hidden, bytes_accessed=6 * width * hidden, transcendentals=tokens * hidden
        ),
    )(x, wg, wu, wd)


def backward_kernel(dg, du, wg, wu, h, dy, dh, by_gate, by_up):
    j = pl.program_id(0)
    tiles = h.shape[0] // TILE

    @pl.when(j == 0)
    def _():
        def start(here):
            by_gate[here] = jnp.zeros((CHUNK, h.shape[1]), F32)
            by_up[here] = jnp.zeros((CHUNK, h.shape[1]), F32)

        rows_of(h, start)

    for i in range(tiles):
        here = pl.ds(i * TILE, TILE)
        by_gate[here] += dot(dg[here], wg[0], NT)
        by_up[here] += dot(du[here], wu[0], NT)

    @pl.when(j == pl.num_programs(0) - 1)
    def _():
        def finish(here):
            wide = h[here].astype(F32)
            scale = scale_of(wide)
            da = (by_gate[here].astype(BF16) + by_up[here].astype(BF16)).astype(F32)
            along = jnp.mean(da * wide, -1, keepdims=True) * (scale * scale * scale)
            dh[here] = dy[here] + (da * scale - wide * along).astype(BF16)

        rows_of(h, finish)


def backward(layer, dg, du, wg, wu, h, dy):
    tokens, width = h.shape
    hidden = wg.shape[2]
    block = SEG * OWNERS
    whole = pl.BlockSpec(memory_space=pltpu.VMEM)
    across = pl.BlockSpec((1, width, block), lambda j: (layer, 0, j))
    columns = pl.BlockSpec((tokens, block), lambda j: (0, j))
    return pl.pallas_call(
        backward_kernel,
        name="backward",
        grid=(hidden // block,),
        out_shape=jax.ShapeDtypeStruct((tokens, width), BF16),
        in_specs=[columns, columns, across, across, whole, whole],
        out_specs=whole,
        scratch_shapes=[pltpu.VMEM((tokens, width), F32)] * 2,
        compiler_params=pltpu.CompilerParams(vmem_limit_bytes=67043328),
        cost_estimate=pl.CostEstimate(
            flops=4 * tokens * width * hidden, bytes_accessed=4 * width * hidden + 4 * tokens * hidden, transcendentals=0
        ),
    )(dg, du, wg, wu, h, dy)


def place_kernel(layer, parts, *refs):
    sources, (out, buffer, read, write) = refs[: len(parts)], refs[-4:]
    me = lax.axis_index("dp")
    x, y, c = me // 4, (me // 2) % 2, me % 2
    copies = []
    for source, (blocks, index, other) in zip(sources, parts, strict=True):
        core = 1 - c if other else c
        rows = source.shape[0] // blocks
        for i in range(blocks):
            second, first = (index + i) % 2, (index + i) // 2
            x_flip, y_flip = core * second + (1 - core) * first, core * first + (1 - core) * second
            owner = 4 * (x + x_flip - 2 * x * x_flip) + 2 * (y + y_flip - 2 * y * y_flip) + core
            there = pl.multiple_of(owner * rows, 16)
            n = len(copies)
            copies.append(
                (
                    pltpu.make_async_copy(source.at[pl.ds(i * rows, rows)], buffer.at[n], read.at[n]),
                    pltpu.make_async_copy(buffer.at[n], out.at[layer, pl.ds(there, rows)], write.at[n]),
                )
            )
    for first, _ in copies:
        first.start()
    for first, second in copies:
        first.wait()
        second.start()
    for _, second in copies:
        second.wait()


def place(out, layer, *pieces):
    sources, parts = [p[0] for p in pieces], tuple(p[1:] for p in pieces)
    rows, columns = sources[0].shape[0] // parts[0][0], sources[0].shape[1]
    count = sum(p[0] for p in parts)
    anywhere = pl.BlockSpec(memory_space=pl.ANY)
    if out is not None:
        sources.append(out)
    return pl.pallas_call(
        functools.partial(place_kernel, layer, parts),
        name=f"place_{layer}",
        out_shape=jax.ShapeDtypeStruct((2, 8 * rows, columns), BF16),
        in_specs=[anywhere] * len(sources),
        out_specs=anywhere,
        input_output_aliases={} if out is None else {len(parts): 0},
        scratch_shapes=[
            pltpu.VMEM((count, rows, columns), BF16),
            pltpu.SemaphoreType.DMA((count,)),
            pltpu.SemaphoreType.DMA((count,)),
        ],
        compiler_params=pltpu.CompilerParams(vmem_limit_bytes=16 << 20),
        cost_estimate=pl.CostEstimate(flops=count * rows * columns * 1000, bytes_accessed=4 * count * rows * columns, transcendentals=0),
    )(*sources)


def moments_kernel(m, v, g0, g1, new_m, new_v):
    first = pl.program_id(0) == 0
    g = jnp.where(first, g0[...], g1[...]).astype(F32)
    new_m[0] = 0.9 * m[0] + 0.1 * g
    new_v[0] = 0.95 * v[0] + 0.05 * g * g


def moments_of(m, v, g0, g1):
    layers, rows, columns = m.shape
    count = rows // 4 if rows % 64 == 0 else rows // 5
    wide = pl.BlockSpec((1, count, columns), lambda layer, i: (layer, i, 0))
    narrow = pl.BlockSpec((count, columns), lambda layer, i: (i, 0))
    return pl.pallas_call(
        moments_kernel,
        name="moments",
        grid=(layers, rows // count),
        out_shape=[jax.ShapeDtypeStruct(m.shape, F32)] * 2,
        in_specs=[wide, wide, narrow, narrow],
        out_specs=[wide, wide],
        compiler_params=pltpu.CompilerParams(vmem_limit_bytes=24 << 20),
        cost_estimate=pl.CostEstimate(flops=m.size * 500, bytes_accessed=18 * m.size, transcendentals=0),
    )(m, v, g0, g1)


def solution(mesh):
    n = mesh.shape["dp"]

    def pairs(on_core_0, on_core_1):
        return [(i, i ^ (on_core_1 if i % 2 else on_core_0)) for i in range(n)]

    to_second, to_first, to_core = pairs(2, 4), pairs(4, 2), pairs(1, 1)

    def step(x, dy, w_gate, w_up, w_down, *moments):
        weights = (w_gate, w_up, w_down)
        x, dy = x[0], dy[0]
        me = lax.axis_index("dp")

        def new_weight(layer, which, g):
            w = weights[which]
            rows = w.shape[1] // n
            own = lax.dynamic_slice(w, (layer, me * rows, 0), (1, rows, w.shape[2]))[0].astype(F32)
            return adamw(own, moments[which][layer], moments[3 + which][layer], g.astype(F32))[0]

        def wait_for(*arrays):
            return lax.optimization_barrier(arrays)

        def send(array, to):
            return lax.ppermute(array, "dp", to)

        a0, h1, a1 = forward(0, x, *weights)
        gg1, gu1, gd1, dg, du = layer_gradients(1, True, a1, dy, *weights)
        own1 = [new_weight(1, which, g) for which, g in ((0, gg1), (1, gu1), (2, gd1))]
        dg, du, *own1 = wait_for(dg, du, *own1)
        got1 = [send(own, to_second) for own in own1]
        dh1 = backward(1, dg, du, w_gate, w_up, h1, dy)
        dh1, *got1 = wait_for(dh1, *got1)
        two1 = [jnp.concatenate([own, got]) for own, got in zip(own1, got1)]
        more1 = [send(two, to_first) for two in two1]
        gg0, gu0, gd0 = layer_gradients(0, False, a0, dh1, *weights)
        gg0, gu0, gd0, *more1 = wait_for(gg0, gu0, gd0, *more1)
        own0 = [new_weight(0, which, g) for which, g in ((0, gg0), (1, gu0), (2, gd0))]
        gg0, gu0, gd0, own0[0], own0[1], own0[2], *more1 = wait_for(gg0, gu0, gd0, *own0, *more1)
        got0 = [send(own, to_second) for own in own0]
        new = [moments_of(moments[i], moments[3 + i], *g) for i, g in enumerate(((gg0, gg1), (gu0, gu1), (gd0, gd1)))]
        out = [place(None, 1, (two, 2, 0, False), (more, 2, 2, False)) for two, more in zip(two1, more1)]
        got0[0], *done = wait_for(got0[0], *(array for pair in new for array in pair))
        new = [tuple(done[i : i + 2]) for i in (0, 2, 4)]
        other1 = [(send(two, to_core), send(more, to_core)) for two, more in zip(two1, more1)]
        two0, more0 = [None] * 3, [None] * 3
        for i in range(3):
            if i:
                got0[i], out[i - 1] = wait_for(got0[i], out[i - 1])
            two0[i] = jnp.concatenate([own0[i], got0[i]])
            more0[i] = send(two0[i], to_first)
        for i in range(3):
            (two, more), there = other1[i], send(two0[i], to_core)
            out[i] = place(out[i], 1, (two, 2, 0, True), (more, 2, 2, True))
            out[i] = place(out[i], 0, (two0[i], 2, 0, False), (there, 2, 0, True))
            more0[i], out[i] = wait_for(more0[i], out[i])
            out[i] = place(out[i], 0, (more0[i], 2, 2, False), (send(more0[i], to_core), 2, 2, True))
        return (*out, *(m for m, _ in new), *(v for _, v in new))

    seq, whole, block, group = P(("rep", "dp"), None, None), P(None, None, None), P(None, "dp", None), P("rep", None, None)
    return jax.shard_map(
        step,
        mesh=mesh,
        in_specs=(seq, seq) + (whole,) * 3 + (block,) * 6,
        out_specs=(group,) * 3 + (P("rep", "dp", None),) * 6,
        check_vma=False,
    )
```

```python
import functools

import jax
import jax.numpy as jnp
from jax import lax
from jax.experimental import pallas as pl
from jax.experimental.pallas import tpu as pltpu
from jax.sharding import PartitionSpec as P

F32, BF16 = jnp.float32, jnp.bfloat16
MESH = pl.DeviceIdType.MESH
NN, NT, TN = ((1,), (0,)), ((1,), (1,)), ((0,), (0,))

VMEM = 67043328
TILE = 512
SEG = 128
OWNERS = 4
CHUNK = 16


def dot(a, b, dims):
    return lax.dot_general(a, b, (dims, ((), ())), preferred_element_type=F32)


def layer_kernel(layer, save, *refs):
    refs = list(refs)
    a, cot, wg, wu, wd = refs[:5]
    gg, gu, gd = refs[5:8]
    del refs[:8]
    if save:
        dgo, duo = refs[:2]
        del refs[:2]
    (a_v, at_v, cot_v, wg_v, wu_v, wd_v, act_v, dg_v, du_v, t0, t1) = refs[:11]
    del refs[:11]
    (dk, ds0, dr0, ds1, dr1, ds2, dr2) = refs[:7]
    del refs[:7]
    (k, s0, r0, s1, r1, s2, r2) = refs[:7]
    del refs[:7]
    (in_sem, w_sem, save_sem, d_send, d_recv, send, recv, d_free, free) = refs

    tokens, width = a.shape
    hidden = wg.shape[2]
    block = SEG * OWNERS
    blocks = hidden // block
    part = hidden // (2 * OWNERS)
    rows = width // (2 * OWNERS)
    tiles = tokens // TILE
    temp = (t0, t1)

    me = lax.axis_index("dp")
    group = lax.axis_index("rep")
    x, y, c = me // 4, (me // 2) % 2, me % 2
    over_x, over_y = me + 4 - 8 * x, me + 2 - 4 * y
    peers = (me + 1 - 2 * c, (1 - c) * over_x + c * over_y, (1 - c) * over_y + c * over_x)
    first = (1 - c) * x + c * y
    second = (1 - c) * y + c * x

    def at_peer(stage):
        return (group, peers[stage])

    def columns(j, p):
        kind = j % 2
        swapped = (p % 2) * 2 + p // 2
        chip = p + kind * (swapped - p)
        return pl.multiple_of((2 * chip + kind) * part + (j // 2) * SEG, SEG)

    def load_weights(j):
        for p in range(OWNERS):
            here = pl.ds(columns(j, p), SEG)
            there = pl.ds(p * SEG, SEG)
            pltpu.make_async_copy(wg.at[layer, :, here], wg_v.at[:, there], w_sem.at[0]).start()
            pltpu.make_async_copy(wu.at[layer, :, here], wu_v.at[:, there], w_sem.at[1]).start()
            pltpu.make_async_copy(wd.at[layer, here], wd_v.at[there], w_sem.at[2]).start()

    def wait_weights():
        for i, buffer in enumerate((wg_v, wu_v, wd_v)):
            pltpu.make_async_copy(buffer, buffer, w_sem.at[i]).wait()

    def input_copies(i):
        here = pl.ds(i * TILE, TILE)
        return (
            pltpu.make_async_copy(a.at[here], a_v.at[here], in_sem.at[0, i]),
            pltpu.make_async_copy(cot.at[here], cot_v.at[here], in_sem.at[1, i]),
        )

    def save_copies(j):
        copies = []
        for p in range(OWNERS):
            here, there = pl.ds(columns(j, p), SEG), pl.ds(p * SEG, SEG)
            copies.append(pltpu.make_async_copy(dg_v.at[:, there], dgo.at[:, here], save_sem.at[0, p]))
            copies.append(pltpu.make_async_copy(du_v.at[:, there], duo.at[:, here], save_sem.at[1, p]))
        return copies

    load_weights(0)
    for i in range(tiles):
        for copy in input_copies(i):
            copy.start()

    barrier = pltpu.get_barrier_semaphore()
    for stage in range(3):
        pl.semaphore_signal(barrier, inc=1, device_id=at_peer(stage), device_id_type=MESH)
    pl.semaphore_wait(barrier, 3)

    def turn(i):
        here = pl.ds(i * TILE, TILE)
        turned = a_v[here].T
        for o in range(2 * OWNERS):
            place = (o // 4) * 2 + (o // 2) % 2 if o % 2 == 0 else (o // 2) % 2 * 2 + o // 4
            at_v[o % 2, place * rows : (place + 1) * rows, here] = turned[o * rows : (o + 1) * rows]

    def project(i):
        here = pl.ds(i * TILE, TILE)
        t = temp[i % 2]
        t[0] = dot(a_v[here], wg_v[...], NN)
        t[1] = dot(a_v[here], wu_v[...], NN)
        t[2] = dot(cot_v[here], wd_v[...], NT)

    def through_product(i):
        t = temp[i % 2]
        for r in range(0, TILE, CHUNK):
            here = pl.ds(r, CHUNK)
            there = pl.ds(i * TILE + r, CHUNK)
            gate, up = t[0, here], t[1, here]
            d = t[2, here].astype(BF16).astype(F32)
            s = 1.0 / (1.0 + jnp.exp(-gate))
            silu = gate * s
            act_v[there] = (silu * up).astype(BF16)
            du_v[there] = (d * silu).astype(BF16)
            dg_v[there] = (d * up * (s + silu * (1.0 - s))).astype(BF16)

    half, quarter = block // 2, block // 4
    d_first = pl.multiple_of(first * half, half)
    d_away = pl.multiple_of((1 - first) * half, half)
    d_second = pl.multiple_of(second * quarter, quarter)
    d_other = pl.multiple_of((1 - second) * quarter, quarter)

    def d_copy(stage):
        source, target = ((ds0, dr0), (ds1, dr1), (ds2, dr2))[stage]
        return pltpu.make_async_remote_copy(
            source, target, d_send.at[stage], d_recv.at[stage], device_id=at_peer(stage), device_id_type=MESH
        )

    def d_start(j, stage):
        @pl.when(j >= 2)
        def _():
            pl.semaphore_wait(d_free.at[stage], 1)

        d_copy(stage).start()

    def d_term(j):
        dk[j % 2] = dot(act_v[...], cot_v[...], TN)

        @pl.when(j % 2 != c)
        def _():
            ds0[...] = dk[j % 2].astype(BF16)
            d_start(j, 0)

    def d_one(j):
        @pl.when(j % 2 != c)
        def _():
            d_copy(0).wait_send()

        @pl.when(j % 2 == c)
        def _():
            d_copy(0).wait_recv()
            here = pl.ds(d_away, half)
            ds1[...] = (dk[c, here] + dr0[here].astype(F32)).astype(BF16)
            d_start(j, 1)

    def d_two(j):
        @pl.when(j % 2 == c)
        def _():
            d_copy(1).wait()
            here = pl.ds(pl.multiple_of(d_first + d_other, quarter), quarter)
            ds2[...] = (dk[c, here] + dr0[here].astype(F32) + dr1[pl.ds(d_other, quarter)].astype(F32)).astype(BF16)
            d_start(j, 2)

    def d_three(j):
        @pl.when(j % 2 == c)
        def _():
            d_copy(2).wait()
            here = pl.ds(pl.multiple_of(d_first + d_second, quarter), quarter)
            total = dk[c, here] + dr0[here].astype(F32) + dr1[pl.ds(d_second, quarter)].astype(F32) + dr2[...].astype(F32)
            gd[pl.ds(pl.multiple_of((j // 2) * SEG, SEG), SEG)] = total.astype(BF16)

            @pl.when(j + 2 < blocks)
            def _():
                for stage in range(3):
                    pl.semaphore_signal(d_free.at[stage], inc=1, device_id=at_peer(stage), device_id_type=MESH)

    first_rows = pl.multiple_of(first * 2 * rows, 2 * rows)
    away_rows = pl.multiple_of((1 - first) * 2 * rows, 2 * rows)
    second_rows = pl.multiple_of(second * rows, rows)
    other_rows = pl.multiple_of((1 - second) * rows, rows)

    def copy_of(j, w, stage):
        slot = j % 2
        source, target = ((s0, r0), (s1, r1), (s2, r2))[stage]
        return pltpu.make_async_remote_copy(
            source.at[w, slot],
            target.at[w, slot],
            send.at[w, slot, stage],
            recv.at[w, slot, stage],
            device_id=at_peer(stage),
            device_id_type=MESH,
        )

    def start(j, w, stage):
        @pl.when(j >= 2)
        def _():
            pl.semaphore_wait(free.at[w, stage], 1)

        copy_of(j, w, stage).start()

    def term_away(j, w):
        s0[w, j % 2] = dot(at_v[1 - c], (dg_v, du_v)[w][...], NN).astype(BF16)
        start(j, w, 0)

    def term_kept(j, w):
        k[w, j % 2] = dot(at_v[c], (dg_v, du_v)[w][...], NN)

    def one(j, w):
        slot = j % 2
        copy_of(j, w, 0).wait()
        here = pl.ds(away_rows, 2 * rows)
        s1[w, slot] = (k[w, slot, here] + r0[w, slot, here].astype(F32)).astype(BF16)
        start(j, w, 1)

    def two(j, w):
        slot = j % 2
        copy_of(j, w, 1).wait()
        here = pl.ds(pl.multiple_of(first_rows + other_rows, rows), rows)
        s2[w, slot] = (
            k[w, slot, here] + r0[w, slot, here].astype(F32) + r1[w, slot, pl.ds(other_rows, rows)].astype(F32)
        ).astype(BF16)
        start(j, w, 2)

    def three(j, w):
        slot = j % 2
        copy_of(j, w, 2).wait()
        here = pl.ds(pl.multiple_of(first_rows + second_rows, rows), rows)
        there = pl.ds(second_rows, rows)
        for p in range(OWNERS):
            at_p = pl.ds(p * SEG, SEG)
            total = (
                k[w, slot, here, at_p]
                + r0[w, slot, here, at_p].astype(F32)
                + r1[w, slot, there, at_p].astype(F32)
                + r2[w, slot, :, at_p].astype(F32)
            )
            (gg, gu)[w][:, pl.ds(columns(j, p), SEG)] = total.astype(BF16)

        @pl.when(j + 2 < blocks)
        def _():
            for stage in range(3):
                pl.semaphore_signal(free.at[w, stage], inc=1, device_id=at_peer(stage), device_id_type=MESH)

    g, u = 0, 1

    def step(j, carry):
        def after(event, back, *args):
            @pl.when(j >= back)
            def _():
                event(j - back, *args)

        wait_weights()
        for i in range(tiles):

            @pl.when(j == 0)
            def _():
                for copy in input_copies(i):
                    copy.wait()
                turn(i)

            if save and i == 1:

                @pl.when(j >= 1)
                def _():
                    for copy in save_copies(j - 1):
                        copy.wait()

            project(i)
            if i >= 1:
                through_product(i - 1)
            if i == 0:
                after(one, 1, u)
                after(three, 2, g)
            if i == 1:
                after(three, 2, u)
            if i == tiles - 1:
                after(d_two, 1)

        @pl.when(j + 1 < blocks)
        def _():
            load_weights(j + 1)

        through_product(tiles - 1)
        if save:
            for copy in save_copies(j):
                copy.start()

        d_term(j)
        after(two, 1, g)
        term_away(j, g)
        term_kept(j, g)
        after(two, 1, u)
        d_one(j)
        term_away(j, u)
        one(j, g)
        after(d_three, 1)
        term_kept(j, u)
        return carry

    lax.fori_loop(0, blocks, step, 0)
    last = blocks - 1
    one(last, u)
    three(last - 1, g)
    three(last - 1, u)
    d_two(last)
    two(last, g)
    two(last, u)
    d_three(last)
    three(last, g)
    three(last, u)
    if save:
        for copy in save_copies(last):
            copy.wait()


def layer_gradients(layer, save, a, cot, wg, wu, wd):
    tokens, width = a.shape
    hidden = wg.shape[2]
    block = SEG * OWNERS
    rows, part = width // (2 * OWNERS), hidden // (2 * OWNERS)
    half, quarter = block // 2, block // 4
    anywhere, vmem = pl.BlockSpec(memory_space=pl.ANY), pl.BlockSpec(memory_space=pltpu.VMEM)
    out_shape = [
        jax.ShapeDtypeStruct((rows, hidden), BF16),
        jax.ShapeDtypeStruct((rows, hidden), BF16),
        jax.ShapeDtypeStruct((part, width), BF16),
    ]
    out_specs = [vmem] * 3
    if save:
        out_shape += [jax.ShapeDtypeStruct((tokens, hidden), BF16)] * 2
        out_specs += [anywhere] * 2
    dma, regular = pltpu.SemaphoreType.DMA, pltpu.SemaphoreType.REGULAR
    return pl.pallas_call(
        functools.partial(layer_kernel, layer, save),
        name=f"layer_{layer}",
        out_shape=out_shape,
        in_specs=[anywhere] * 5,
        out_specs=out_specs,
        scratch_shapes=[
            pltpu.VMEM((tokens, width), BF16),
            pltpu.VMEM((2, width // 2, tokens), BF16),
            pltpu.VMEM((tokens, width), BF16),
            pltpu.VMEM((width, block), BF16),
            pltpu.VMEM((width, block), BF16),
            pltpu.VMEM((block, width), BF16),
            pltpu.VMEM((tokens, block), BF16),
            pltpu.VMEM((tokens, block), BF16),
            pltpu.VMEM((tokens, block), BF16),
            pltpu.VMEM((3, TILE, block), F32),
            pltpu.VMEM((3, TILE, block), F32),
            pltpu.VMEM((2, block, width), F32),
            pltpu.VMEM((block, width), BF16),
            pltpu.VMEM((block, width), BF16),
            pltpu.VMEM((half, width), BF16),
            pltpu.VMEM((half, width), BF16),
            pltpu.VMEM((quarter, width), BF16),
            pltpu.VMEM((quarter, width), BF16),
            pltpu.VMEM((2, 2, 4 * rows, block), F32),
            pltpu.VMEM((2, 2, 4 * rows, block), BF16),
            pltpu.VMEM((2, 2, 4 * rows, block), BF16),
            pltpu.VMEM((2, 2, 2 * rows, block), BF16),
            pltpu.VMEM((2, 2, 2 * rows, block), BF16),
            pltpu.VMEM((2, 2, rows, block), BF16),
            pltpu.VMEM((2, 2, rows, block), BF16),
            dma((2, tokens // TILE)),
            dma((3,)),
            dma((2, OWNERS)),
            dma((3,)),
            dma((3,)),
            dma((2, 2, 3)),
            dma((2, 2, 3)),
            regular((3,)),
            regular((2, 3)),
        ],
        compiler_params=pltpu.CompilerParams(
            collective_id=layer, has_side_effects=True, vmem_limit_bytes=VMEM
        ),
        cost_estimate=pl.CostEstimate(
            flops=12 * tokens * width * hidden, bytes_accessed=10 * width * hidden, transcendentals=tokens * hidden
        ),
    )(a, cot, wg, wu, wd)


def rows_of(ref, body):
    def step(i, carry):
        body(pl.ds(pl.multiple_of(i * CHUNK, CHUNK), CHUNK))
        return carry

    lax.fori_loop(0, ref.shape[0] // CHUNK, step, 0, unroll=4)


def scale_of(wide):
    return lax.rsqrt(jnp.mean(wide * wide, -1, keepdims=True) + 1e-6)


def forward_kernel(x, wg, wu, wd, a0, h1, a1, total, act, t0, t1):
    j = pl.program_id(0)
    temp = (t0, t1)
    tiles = x.shape[0] // TILE

    @pl.when(j == 0)
    def _():
        def start(here):
            wide = x[here].astype(F32)
            a0[here] = (wide * scale_of(wide)).astype(BF16)
            total[here] = jnp.zeros_like(wide)

        rows_of(x, start)

    def product(i):
        for r in range(0, TILE, CHUNK):
            gate, up = temp[i % 2][0, pl.ds(r, CHUNK)], temp[i % 2][1, pl.ds(r, CHUNK)]
            s = 1.0 / (1.0 + jnp.exp(-gate))
            act[i % 2, pl.ds(r, CHUNK)] = (gate * s * up).astype(BF16)

    def down(i):
        total[pl.ds(i * TILE, TILE)] += dot(act[i % 2], wd[0], NN)

    for i in range(tiles):
        here = pl.ds(i * TILE, TILE)
        temp[i % 2][0] = dot(a0[here], wg[0], NN)
        temp[i % 2][1] = dot(a0[here], wu[0], NN)
        if i >= 1:
            product(i - 1)
        if i >= 2:
            down(i - 2)
    product(tiles - 1)
    down(tiles - 2)
    down(tiles - 1)

    @pl.when(j == pl.num_programs(0) - 1)
    def _():
        def finish(here):
            h = x[here] + total[here].astype(BF16)
            h1[here] = h
            wide = h.astype(F32)
            a1[here] = (wide * scale_of(wide)).astype(BF16)

        rows_of(x, finish)


def forward(layer, x, wg, wu, wd):
    tokens, width = x.shape
    hidden = wg.shape[2]
    block = SEG * OWNERS
    whole = pl.BlockSpec(memory_space=pltpu.VMEM)
    across = pl.BlockSpec((1, width, block), lambda j: (layer, 0, j))
    return pl.pallas_call(
        forward_kernel,
        name="forward",
        grid=(hidden // block,),
        out_shape=[jax.ShapeDtypeStruct((tokens, width), BF16)] * 3,
        in_specs=[whole, across, across, pl.BlockSpec((1, block, width), lambda j: (layer, j, 0))],
        out_specs=[whole] * 3,
        scratch_shapes=[
            pltpu.VMEM((tokens, width), F32),
            pltpu.VMEM((2, TILE, block), BF16),
            pltpu.VMEM((2, TILE, block), F32),
            pltpu.VMEM((2, TILE, block), F32),
        ],
        compiler_params=pltpu.CompilerParams(vmem_limit_bytes=VMEM),
        cost_estimate=pl.CostEstimate(
            flops=6 * tokens * width * hidden, bytes_accessed=6 * width * hidden, transcendentals=tokens * hidden
        ),
    )(x, wg, wu, wd)


def backward_kernel(dg, du, wg, wu, h, dy, dh, by_gate, by_up):
    j = pl.program_id(0)
    tiles = h.shape[0] // TILE

    @pl.when(j == 0)
    def _():
        def start(here):
            by_gate[here] = jnp.zeros((CHUNK, h.shape[1]), F32)
            by_up[here] = jnp.zeros((CHUNK, h.shape[1]), F32)

        rows_of(h, start)

    for i in range(tiles):
        here = pl.ds(i * TILE, TILE)
        by_gate[here] += dot(dg[here], wg[0], NT)
        by_up[here] += dot(du[here], wu[0], NT)

    @pl.when(j == pl.num_programs(0) - 1)
    def _():
        def finish(here):
            wide = h[here].astype(F32)
            scale = scale_of(wide)
            da = (by_gate[here].astype(BF16) + by_up[here].astype(BF16)).astype(F32)
            along = jnp.mean(da * wide, -1, keepdims=True) * (scale * scale * scale)
            dh[here] = dy[here] + (da * scale - wide * along).astype(BF16)

        rows_of(h, finish)


def backward(layer, dg, du, wg, wu, h, dy):
    tokens, width = h.shape
    hidden = wg.shape[2]
    block = SEG * OWNERS
    whole = pl.BlockSpec(memory_space=pltpu.VMEM)
    across = pl.BlockSpec((1, width, block), lambda j: (layer, 0, j))
    columns = pl.BlockSpec((tokens, block), lambda j: (0, j))
    return pl.pallas_call(
        backward_kernel,
        name="backward",
        grid=(hidden // block,),
        out_shape=jax.ShapeDtypeStruct((tokens, width), BF16),
        in_specs=[columns, columns, across, across, whole, whole],
        out_specs=whole,
        scratch_shapes=[pltpu.VMEM((tokens, width), F32)] * 2,
        compiler_params=pltpu.CompilerParams(vmem_limit_bytes=VMEM),
        cost_estimate=pl.CostEstimate(
            flops=4 * tokens * width * hidden, bytes_accessed=4 * width * hidden + 4 * tokens * hidden, transcendentals=0
        ),
    )(dg, du, wg, wu, h, dy)


def place_kernel(layer, parts, *refs):
    sources, (out, buffer, read, write) = refs[: len(parts)], refs[-4:]
    me = lax.axis_index("dp")
    x, y, c = me // 4, (me // 2) % 2, me % 2
    copies = []
    for source, (blocks, index, other) in zip(sources, parts, strict=True):
        core = 1 - c if other else c
        rows = source.shape[0] // blocks
        for i in range(blocks):
            second, first = (index + i) % 2, (index + i) // 2
            x_flip, y_flip = core * second + (1 - core) * first, core * first + (1 - core) * second
            owner = 4 * (x + x_flip - 2 * x * x_flip) + 2 * (y + y_flip - 2 * y * y_flip) + core
            there = pl.multiple_of(owner * rows, 16)
            n = len(copies)
            copies.append(
                (
                    pltpu.make_async_copy(source.at[pl.ds(i * rows, rows)], buffer.at[n], read.at[n]),
                    pltpu.make_async_copy(buffer.at[n], out.at[layer, pl.ds(there, rows)], write.at[n]),
                )
            )
    for first, _ in copies:
        first.start()
    for first, second in copies:
        first.wait()
        second.start()
    for _, second in copies:
        second.wait()


def place(out, layer, *pieces):
    sources, parts = [p[0] for p in pieces], tuple(p[1:] for p in pieces)
    rows, columns = sources[0].shape[0] // parts[0][0], sources[0].shape[1]
    count = sum(p[0] for p in parts)
    anywhere = pl.BlockSpec(memory_space=pl.ANY)
    if out is not None:
        sources.append(out)
    return pl.pallas_call(
        functools.partial(place_kernel, layer, parts),
        name=f"place_{layer}",
        out_shape=jax.ShapeDtypeStruct((2, 8 * rows, columns), BF16),
        in_specs=[anywhere] * len(sources),
        out_specs=anywhere,
        input_output_aliases={} if out is None else {len(parts): 0},
        scratch_shapes=[
            pltpu.VMEM((count, rows, columns), BF16),
            pltpu.SemaphoreType.DMA((count,)),
            pltpu.SemaphoreType.DMA((count,)),
        ],
        compiler_params=pltpu.CompilerParams(vmem_limit_bytes=VMEM),
        cost_estimate=pl.CostEstimate(flops=count * rows * columns * 1000, bytes_accessed=4 * count * rows * columns, transcendentals=0),
    )(*sources)


def new_weight_kernel(me, w, m, v, g, new):
    g = g[...].astype(F32)
    m = 0.9 * m[0] + 0.1 * g
    v = 0.95 * v[0] + 0.05 * g * g
    w = w[0].astype(F32)
    new[...] = (w - 0.02 * (m * lax.rsqrt(v + 1e-8) + 0.1 * w)).astype(BF16)


def new_weight(layer, me, w, m, v, g):
    rows, columns = g.shape
    count = 4 if rows % 64 == 0 else 5
    tile = rows // count
    moment = pl.BlockSpec((1, tile, columns), lambda i, me: (layer, i, 0))
    own = pl.BlockSpec((tile, columns), lambda i, me: (i, 0))
    return pl.pallas_call(
        new_weight_kernel,
        name=f"new_weight_{layer}",
        out_shape=jax.ShapeDtypeStruct((rows, columns), BF16),
        grid_spec=pltpu.PrefetchScalarGridSpec(
            num_scalar_prefetch=1,
            grid=(count,),
            in_specs=[
                pl.BlockSpec((1, tile, columns), lambda i, me: (layer, me[0] * count + i, 0)),
                moment,
                moment,
                own,
            ],
            out_specs=own,
        ),
        compiler_params=pltpu.CompilerParams(vmem_limit_bytes=VMEM),
        cost_estimate=pl.CostEstimate(flops=g.size * 500, bytes_accessed=14 * g.size, transcendentals=g.size),
    )(me, w, m, v, g)


def moments_kernel(m, v, g0, g1, new_m, new_v):
    first = pl.program_id(0) == 0
    g = jnp.where(first, g0[...], g1[...]).astype(F32)
    new_m[0] = 0.9 * m[0] + 0.1 * g
    new_v[0] = 0.95 * v[0] + 0.05 * g * g


def moments_of(m, v, g0, g1):
    layers, rows, columns = m.shape
    count = rows // 4 if rows % 64 == 0 else rows // 5
    wide = pl.BlockSpec((1, count, columns), lambda layer, i: (layer, i, 0))
    narrow = pl.BlockSpec((count, columns), lambda layer, i: (i, 0))
    return pl.pallas_call(
        moments_kernel,
        name="moments",
        grid=(layers, rows // count),
        out_shape=[jax.ShapeDtypeStruct(m.shape, F32)] * 2,
        in_specs=[wide, wide, narrow, narrow],
        out_specs=[wide, wide],
        compiler_params=pltpu.CompilerParams(vmem_limit_bytes=VMEM),
        cost_estimate=pl.CostEstimate(flops=m.size * 500, bytes_accessed=18 * m.size, transcendentals=0),
    )(m, v, g0, g1)


def solution(mesh):
    n = mesh.shape["dp"]

    def pairs(on_core_0, on_core_1):
        return [(i, i ^ (on_core_1 if i % 2 else on_core_0)) for i in range(n)]

    to_second, to_first, to_core = pairs(2, 4), pairs(4, 2), pairs(1, 1)

    def step(x, dy, w_gate, w_up, w_down, *moments):
        weights = (w_gate, w_up, w_down)
        x, dy = x[0], dy[0]
        me = lax.axis_index("dp").reshape(1)

        def new(layer, which, g):
            return new_weight(layer, me, weights[which], moments[which], moments[3 + which], g)

        def wait_for(*arrays):
            return lax.optimization_barrier(arrays)

        def send(array, to):
            return lax.ppermute(array, "dp", to)

        every = range(3)
        a0, h1, a1 = forward(0, x, *weights)
        *g1, dg, du = layer_gradients(1, True, a1, dy, *weights)
        own1 = [new(1, i, g1[i]) for i in every]
        dg, du, *own1 = wait_for(dg, du, *own1)
        second1, first1 = [send(own, to_second) for own in own1], [send(own, to_first) for own in own1]
        dh1 = backward(1, dg, du, w_gate, w_up, h1, dy)
        dh1, *second1 = wait_for(dh1, *second1)
        both1 = [send(got, to_first) for got in second1]
        g0 = layer_gradients(0, False, a0, dh1, *weights)
        *g0, first1[0], first1[1], first1[2], both1[0], both1[1], both1[2] = wait_for(*g0, *first1, *both1)
        own0, second0, first0 = [None] * 3, [None] * 3, [None] * 3
        for i in every:
            own0[i] = new(0, i, g0[i])
            second0[i], first0[i] = send(own0[i], to_second), send(own0[i], to_first)
        g0 = wait_for(*g0, *own0)[:3]
        after = [moments_of(moments[i], moments[3 + i], g0[i], g1[i]) for i in every]
        chip1 = [(own1[i], second1[i], first1[i], both1[i]) for i in every]
        chip1 = [wait_for(*pieces, own0[2])[:4] for pieces in chip1]
        out = [place(None, 1, *((p, 1, n, False) for n, p in enumerate(chip1[i]))) for i in every]
        both0 = [None] * 3
        for i in every:
            second0[i], *done = wait_for(second0[i], *after[i])
            after[i] = done
            both0[i] = send(second0[i], to_first)
        for i in every:
            there = [send(p, to_core) for p in chip1[i]]
            out[i] = place(out[i], 1, *((p, 1, n, True) for n, p in enumerate(there)))
        for i in every:
            chip = (own0[i], second0[i], first0[i])
            there = [send(p, to_core) for p in chip]
            out[i] = place(out[i], 0, *((p, 1, n, False) for n, p in enumerate(chip)), *((p, 1, n, True) for n, p in enumerate(there)))
        for i in every:
            both0[i], out[i] = wait_for(both0[i], out[i])
            out[i] = place(out[i], 0, (both0[i], 1, 3, False), (send(both0[i], to_core), 1, 3, True))
        return (*out, *(m for m, _ in after), *(v for _, v in after))

    seq, whole, block, group = P(("rep", "dp"), None, None), P(None, None, None), P(None, "dp", None), P("rep", None, None)
    return jax.shard_map(
        step,
        mesh=mesh,
        in_specs=(seq, seq) + (whole,) * 3 + (block,) * 6,
        out_specs=(group,) * 3 + (P("rep", "dp", None),) * 6,
        check_vma=False,
    )
```
